8 devices in a mesh: dp: 2 (over y, z), sp: 4 (over x, core).
Axes of the slice: x: 2, y: 2, z: 1, core: 2. Of those that a mesh axis runs over, the one named last changes fastest.
Arguments:
- q: bfloat16 [64, 96, 128], P('dp'), parts along dimension 0
- k: bfloat16 [64, 8192, 8, 128], P('dp', 'sp'), parts along dimension 0
- v: bfloat16 [64, 8192, 8, 128], P('dp', 'sp'), parts along dimension 0
Outputs:
- q: bfloat16 [64, 96, 128], P('dp'), parts along dimension 0
There are 2 independent parts. The reference program is written for one: setup_inputs(seed, part) draws one part's arguments, and reference() takes and returns one part's arrays. A program takes and returns all parts, laid end to end along the dimension named above; each array names one.
All inputs are finite; a program needn't handle non-finite values.
Results may differ from the reference program's by a relative error of at most 0.012.
Values are sent between devices in bfloat16 or wider.
A program may use at most 2 GiB of HBM per device.

```python
import jax
import jax.numpy as jnp

BATCH = 32
CACHE = 8192
HEADS = 96
KV_HEADS = 8
HEAD = 128


def setup_inputs(seed: int = 0, part: int = 0) -> dict:
    kq, kk, kv = (jax.random.fold_in(k, part) for k in jax.random.split(jax.random.key(seed), 3))
    return {
        "q": (3 * jax.random.normal(kq, (BATCH, HEADS, HEAD), jnp.float32)).astype(jnp.bfloat16),
        "k": jax.random.normal(kk, (BATCH, CACHE, KV_HEADS, HEAD), jnp.float32).astype(jnp.bfloat16),
        "v": jax.random.normal(kv, (BATCH, CACHE, KV_HEADS, HEAD), jnp.float32).astype(jnp.bfloat16),
    }


def einsum(form, a, b):
    return jnp.einsum(form, a.astype(jnp.float32), b.astype(jnp.float32))


def reference(q, k, v):
    grouped = q.reshape(BATCH, KV_HEADS, -1, HEAD)
    scores = einsum("bgsd,bugd->bgsu", grouped, k) * HEAD**-0.5
    weights = jax.nn.softmax(scores, -1).astype(jnp.bfloat16)
    return einsum("bgsu,bugd->bgsd", weights, v).astype(jnp.bfloat16).reshape(BATCH, HEADS, HEAD)
```

```python
import jax
import jax.numpy as jnp
from jax import lax
from jax.experimental import pallas as pl
from jax.experimental.pallas import tpu as pltpu
from jax.sharding import PartitionSpec as P

NBUF = 3


def local_attention(q, k, v):
    seqs, heads, head = q.shape
    length, kv_heads = k.shape[1:3]
    share = heads // kv_heads
    half = heads // 2
    pairs = kv_heads // 2
    rows = 2 * length
    scale = head**-0.5 * 1.4426950408889634
    k = k.reshape(seqs, length, pairs, 2, head)
    v = v.reshape(seqs, length, pairs, 2, head)

    def kern(q_ref, k_hbm, v_hbm, o_ref, st_ref, kb, vb, sb, sem):
        def copies(b, slot, a):
            src, dst = ((k_hbm, kb), (v_hbm, vb))[a]
            return [pltpu.make_async_copy(src.at[b, :, i], dst.at[slot, i], sem.at[slot, a, i]) for i in range(pairs)]

        def both(ref, slot, j, lo):
            part = [ref.at[slot, 2 * j + i].reshape(rows, head)[pl.ds(lo, 256), :] for i in range(2)]
            return jnp.concatenate(part, 1)

        for s in range(NBUF - 1):
            for a in range(2):
                for c in copies(s, s, a):
                    c.start()
        row = lax.broadcasted_iota(jnp.int32, (half, 256), 0)
        lane = lax.broadcasted_iota(jnp.int32, (half, 256), 1)
        valid = lax.rem(lax.div(row, share), 2) == lax.rem(lane, 2)
        first = lax.broadcasted_iota(jnp.int32, (half, head), 0) < half // 2

        @pl.loop(0, seqs)
        def _(b):
            slot = lax.rem(b, NBUF)
            nx = b + NBUF - 1

            @pl.when(nx < seqs)
            def _():
                for a in range(2):
                    for c in copies(nx, lax.rem(nx, NBUF), a):
                        c.start()

            for c in copies(b, slot, 0):
                c.wait()
            ms = []
            for j in range(2):
                qj = q_ref[b, pl.ds(half * j, half), :]
                z = jnp.zeros_like(qj)
                q2 = jnp.concatenate([jnp.where(first, qj, z), jnp.where(first, z, qj)], 1)
                mx = jnp.full((half, head), -jnp.inf, jnp.float32)
                for n in range(rows // 256):
                    s = lax.dot_general(q2, both(kb, slot, j, n * 256), (((1,), (1,)), ((), ())), preferred_element_type=jnp.float32)
                    s = jnp.where(valid, s, -jnp.inf)
                    sb[j, :, pl.ds(n * 256, 256)] = s
                    mx = jnp.maximum(mx, jnp.maximum(s[:, :128], s[:, 128:]))
                ms.append(jnp.max(mx, 1, keepdims=True))
            for c in copies(b, slot, 1):
                c.wait()
            for j in range(2):
                l = jnp.zeros((half, head), jnp.float32)
                o = jnp.zeros((half, 256), jnp.float32)
                for n in range(rows // 256):
                    p = jnp.exp2((sb[j, :, pl.ds(n * 256, 256)] - ms[j]) * scale)
                    l = l + p[:, :128] + p[:, 128:]
                    o = o + jnp.dot(p.astype(jnp.bfloat16), both(vb, slot, j, n * 256), preferred_element_type=jnp.float32)
                l = jnp.sum(l, 1, keepdims=True)
                o_ref[b, pl.ds(half * j, half), :] = jnp.where(first, o[:, :head], o[:, head:]).astype(jnp.bfloat16)
                ln = lax.broadcasted_iota(jnp.int32, (half, head), 1)
                st_ref[b, pl.ds(half * j, half), :] = jnp.where(ln == 0, l, ms[j])

    buf = pltpu.VMEM((NBUF, pairs, length, 2, head), jnp.bfloat16)
    o, st = pl.pallas_call(
        kern,
        out_shape=[jax.ShapeDtypeStruct((seqs, heads, head), jnp.bfloat16), jax.ShapeDtypeStruct((seqs, heads, head), jnp.float32)],
        in_specs=[pl.BlockSpec(memory_space=pltpu.VMEM)] + [pl.BlockSpec(memory_space=pl.ANY)] * 2,
        scratch_shapes=[buf, buf, pltpu.VMEM((2, half, rows), jnp.float32), pltpu.SemaphoreType.DMA((NBUF, 2, pairs))],
        compiler_params=pltpu.CompilerParams(vmem_limit_bytes=60 << 20),
    )(q, k, v)
    return o, st[..., 0], st[..., 1]


def solution(mesh):
    def step(q, k, v):
        o, l, m = local_attention(q, k, v)
        o = lax.all_gather(o, "sp").astype(jnp.float32)
        st = lax.all_gather(jnp.stack([l, m]), "sp")
        l, m = st[:, 0], st[:, 1]
        w = jnp.exp2((m - jnp.max(m, 0)) * (q.shape[2] ** -0.5 * 1.4426950408889634))
        return (jnp.sum(o * w[..., None], 0) / jnp.sum(l * w, 0)[..., None]).astype(jnp.bfloat16)

    return jax.shard_map(
        step,
        mesh=mesh,
        in_specs=(P("dp", None, None), P("dp", "sp", None, None), P("dp", "sp", None, None)),
        out_specs=P("dp", None, None),
        check_vma=False,
    )
```

```python
import jax
import jax.numpy as jnp
from jax import lax
from jax.experimental import pallas as pl
from jax.experimental.pallas import tpu as pltpu
from jax.sharding import PartitionSpec as P

AXIS = "sp"
NBUF = 3
LAG = 3
TILE = 16
CHUNK = 256


def attention(q, k, v, devices):
    seqs, heads, head = q.shape
    length, kv_heads = k.shape[1:3]
    share = heads // kv_heads
    half = heads // 2
    pairs = kv_heads // 2
    rows = 2 * length
    runs = TILE // 2
    run = length // runs
    scale = head**-0.5 * 1.4426950408889634
    k = k.reshape(seqs, length, pairs, 2, head)
    v = v.reshape(seqs, length, pairs, 2, head)

    def kern(q_hbm, k_hbm, v_hbm, o_hbm, qb, kb, vb, sb, part, stat, ob, sem, qo_sem, send_sem, recv_sem):
        me = lax.axis_index(AXIS)
        peers = [lax.rem(me + d, devices) for d in range(1, devices)]

        def fetch(b, slot):
            for a, (src, dst) in enumerate(((k_hbm, kb), (v_hbm, vb))):
                for i in range(pairs):
                    for u in range(runs):
                        pltpu.make_async_copy(src.at[b, pl.ds(u * run, run), i], dst.at[slot, i, :, pl.ds(2 * u, 2), :], sem.at[slot, a]).start()

        def fetched(slot, a):
            dst = (kb, vb)[a].at[slot]
            pltpu.make_async_copy(dst, dst, sem.at[slot, a]).wait()

        def both(ref, slot, j, lo):
            return jnp.concatenate([ref.at[slot, 2 * j + i].reshape(rows, head)[pl.ds(lo, CHUNK), :] for i in range(2)], 1)

        def sends(b):
            out = []
            for d, peer in enumerate(peers):
                for a, ref in enumerate((part, stat)):
                    own = ref.at[me, b]
                    out.append(pltpu.make_async_remote_copy(own, own, send_sem.at[d, a], recv_sem.at[b, me, a], device_id={AXIS: peer}))
            return out

        def together(b):
            for d, peer in enumerate(peers):
                for a, ref in enumerate((part, stat)):
                    theirs = ref.at[peer, b]
                    pltpu.make_async_remote_copy(theirs, theirs, send_sem.at[d, a], recv_sem.at[b, peer, a], device_id={AXIS: peer}).wait_recv()
            stats = [stat[p, b] for p in range(devices)]
            high = stats[0][0:1]
            for s in stats[1:]:
                high = jnp.maximum(high, s[0:1])
            w = [jnp.exp2((s[0:1] - high) * scale) for s in stats]
            total = w[0] * stats[0][1:2]
            for p in range(1, devices):
                total = total + w[p] * stats[p][1:2]
            sub = lax.broadcasted_iota(jnp.int32, (8, head), 0)
            table = jnp.zeros((8, head), jnp.float32)
            for p in range(devices):
                table = jnp.where(sub == p, w[p] / total, table)
            table = table.T
            out = part[0, b].astype(jnp.float32) * table[:heads, 0:1]
            for p in range(1, devices):
                out = out + part[p, b].astype(jnp.float32) * table[:heads, p : p + 1]
            ob[b] = out.astype(jnp.bfloat16)
            pltpu.make_async_copy(ob.at[b], o_hbm.at[b], qo_sem.at[1]).start()

        barrier = pltpu.get_barrier_semaphore()
        for peer in peers:
            pl.semaphore_signal(barrier, inc=1, device_id={AXIS: peer})
        fetch_q = pltpu.make_async_copy(q_hbm, qb, qo_sem.at[0])
        fetch_q.start()
        for s in range(NBUF - 1):
            fetch(s, s)
        fetch_q.wait()
        pl.semaphore_wait(barrier, devices - 1)

        row = lax.broadcasted_iota(jnp.int32, (half, CHUNK), 0)
        lane = lax.broadcasted_iota(jnp.int32, (half, CHUNK), 1)
        valid = lax.rem(lax.div(row, share), 2) == lax.rem(lane, 2)
        first = row[:, :head] < half // 2

        @pl.loop(0, seqs)
        def _(b):
            slot = lax.rem(b, NBUF)

            @pl.when(b + NBUF - 1 < seqs)
            def _():
                fetch(b + NBUF - 1, lax.rem(b + NBUF - 1, NBUF))

            @pl.when(b >= LAG)
            def _():
                together(b - LAG)

            fetched(slot, 0)
            highs = []
            for j in range(2):
                qj = qb[b, pl.ds(half * j, half), :]
                zero = jnp.zeros_like(qj)
                q2 = jnp.concatenate([jnp.where(first, qj, zero), jnp.where(first, zero, qj)], 1)
                mx = jnp.full((half, head), -jnp.inf, jnp.float32)
                for n in range(rows // CHUNK):
                    s = lax.dot_general(q2, both(kb, slot, j, n * CHUNK), (((1,), (1,)), ((), ())), preferred_element_type=jnp.float32)
                    s = jnp.where(valid, s, -jnp.inf)
                    sb[j, :, pl.ds(n * CHUNK, CHUNK)] = s
                    mx = jnp.maximum(mx, jnp.maximum(s[:, :head], s[:, head:]))
                highs.append(jnp.max(mx, 1, keepdims=True))
            fetched(slot, 1)
            high_row = jnp.zeros((1, head), jnp.float32)
            total_row = jnp.zeros((1, head), jnp.float32)
            for j in range(2):
                total = jnp.zeros((half, head), jnp.float32)
                seen = jnp.zeros((half, 2 * head), jnp.float32)
                for n in range(rows // CHUNK):
                    w = jnp.exp2((sb[j, :, pl.ds(n * CHUNK, CHUNK)] - highs[j]) * scale)
                    total = total + w[:, :head] + w[:, head:]
                    seen = seen + jnp.dot(w.astype(jnp.bfloat16), both(vb, slot, j, n * CHUNK), preferred_element_type=jnp.float32)
                part[me, b, pl.ds(half * j, half), :] = jnp.where(first, seen[:, :head], seen[:, head:]).astype(jnp.bfloat16)
                own = row[:, :head] + half * j == lane[:, :head]
                high_row = high_row + jnp.sum(jnp.where(own, highs[j], 0.0), 0, keepdims=True)
                total_row = total_row + jnp.sum(jnp.where(own, jnp.sum(total, 1, keepdims=True), 0.0), 0, keepdims=True)
            sub = lax.broadcasted_iota(jnp.int32, (8, head), 0)
            stat[me, b] = jnp.where(sub == 0, high_row, jnp.where(sub == 1, total_row, 0.0))

            @pl.when(b > 0)
            def _():
                for c in sends(b - 1):
                    c.wait_send()

            for c in sends(b):
                c.start()

        @pl.loop(seqs - LAG, seqs)
        def _(b):
            together(b)

        for c in sends(seqs - 1):
            c.wait_send()
        pltpu.make_async_copy(ob, o_hbm, qo_sem.at[1]).wait()

    buf = pltpu.VMEM((NBUF, pairs, rows // TILE, TILE, head), jnp.bfloat16)
    return pl.pallas_call(
        kern,
        out_shape=jax.ShapeDtypeStruct(q.shape, q.dtype),
        in_specs=[pl.BlockSpec(memory_space=pl.ANY)] * 3,
        out_specs=pl.BlockSpec(memory_space=pl.ANY),
        scratch_shapes=[
            pltpu.VMEM(q.shape, q.dtype),
            buf,
            buf,
            pltpu.VMEM((2, half, rows), jnp.float32),
            pltpu.VMEM((devices, seqs, heads, head), jnp.bfloat16),
            pltpu.VMEM((devices, seqs, 8, head), jnp.float32),
            pltpu.VMEM(q.shape, q.dtype),
            pltpu.SemaphoreType.DMA((NBUF, 2)),
            pltpu.SemaphoreType.DMA((2,)),
            pltpu.SemaphoreType.DMA((devices - 1, 2)),
            pltpu.SemaphoreType.DMA((seqs, devices, 2)),
        ],
        compiler_params=pltpu.CompilerParams(vmem_limit_bytes=60 << 20, collective_id=0, has_side_effects=True),
        cost_estimate=pl.CostEstimate(flops=4 * heads * head * length * seqs, bytes_accessed=2 * k.size * 2, transcendentals=heads * length * seqs),
    )(q, k, v)


def solution(mesh):
    return jax.shard_map(
        lambda q, k, v: attention(q, k, v, mesh.shape[AXIS]),
        mesh=mesh,
        in_specs=(P("dp", None, None), P("dp", AXIS, None, None), P("dp", AXIS, None, None)),
        out_specs=P("dp", None, None),
        check_vma=False,
    )
```
